32 devices in a mesh: seq: 32 (over z, y, x, core).
Axes of the slice: x: 2, y: 2, z: 4, core: 2. Of those that a mesh axis runs over, the one named last changes fastest.
Arguments:
- queries: bfloat16 [8192, 8, 128], P('seq'), may hold values from -132 to 132
- keys: bfloat16 [16384, 8, 128], P('seq'), may hold values from -6 to 6
- values: bfloat16 [16384, 8, 128], P('seq'), may hold values from -6 to 6
- routes: int32 [8192, 8], P('seq'), may hold values from 0 to 63, all different within a row; in each aligned block of 256 rows (0 to 255, 256 to 511, ...) at most 40 rows name the same one
Outputs:
- attended: bfloat16 [8192, 8, 128], P('seq')
The draws below stay inside these ranges and needn't reach their ends.
Inputs may be any that keep to these rules, and one draw needn't show every extreme that they name: `routes`: each row names 8 different heads; among the 256 rows of one device no head is named more than 40 times, a bound that some block reaches.
All inputs are finite; a program needn't handle non-finite values.
Results may differ from the reference program's by a relative error of at most 0.0065.
Values may be sent and summed in bfloat16 or wider, within the bound.
A program may use at most 64 MiB of HBM per device.

```python
import math
import jax
import jax.numpy as jnp
import numpy as np
from jax import lax

HEADS = 64
KV_HEADS = 8
HEAD_DIM = 128
ROUTED = 8
HOPS = 4
MOST = 40
QRY_DEV = 256
CTX_DEV = 512
CONTEXT = 16384
QUERIES = 8192


def base_keys(key):
    shards = CONTEXT // CTX_DEV
    normal_keys = jax.random.truncated_normal(jax.random.fold_in(key, 11), -6.0, 6.0, (shards, CTX_DEV, KV_HEADS, HEAD_DIM), jnp.float32)
    return normal_keys


def draw_keys(key, part):
    return base_keys(key).reshape(CONTEXT, KV_HEADS, HEAD_DIM).astype(jnp.bfloat16)


def draw_queries(key, part):
    shards = CONTEXT // CTX_DEV
    drawn = jax.random.truncated_normal(jax.random.fold_in(key, 13), -6.0, 6.0, (shards, QRY_DEV, ROUTED, HEAD_DIM), jnp.float32)
    return drawn.reshape(QUERIES, ROUTED, HEAD_DIM).astype(jnp.bfloat16)


def shard_levels(own_key, extent, cuts, least, high):
    factor_of, own = 1.0, jax.random.fold_in(own_key, 6)
    for axis_at, parts in cuts:
        steps = jnp.exp(jax.random.uniform(jax.random.fold_in(own, axis_at), (parts,), jnp.float32, least / len(cuts), high / len(cuts)))
        factor_of = factor_of * jnp.repeat(steps, extent[axis_at] // parts).reshape([-1 if axis == axis_at else 1 for axis in range(len(extent))])
    return factor_of


def shared_out(rng, own, number, rows, count, top, limit, slope):
    ranking = jax.random.permutation(rng, count)
    crowded, common = load_shares(count, rows * top, limit, slope, True), load_shares(count, rows * top, limit, slope, False)
    places = jnp.arange(count)

    def named(lengths, offset_by):
        used = int((lengths > 0).sum())
        fixed = max(1, used // 4)
        passed = fixed + (places - fixed + offset_by * (used - fixed)) % max(1, count - fixed)
        return jnp.zeros((count,), jnp.int32).at[ranking[jnp.where(places < fixed, places, passed)]].set(jnp.asarray(lengths, jnp.int32))

    lengths = jnp.where(number % 4 == 0, named(crowded, number // 4), named(common, number - number // 4 - 1))
    mixed = jax.random.permutation(jax.random.fold_in(own, 3), count)
    giver, receiver = mixed[0:count // 2 * 2:2], mixed[1:count // 2 * 2:2]
    margin = jnp.minimum(lengths[giver] - 1, limit - lengths[receiver]) // 2
    margin = jnp.where((giver == ranking[0]) | (receiver == ranking[0]) | (lengths[receiver] == 0), 0, jnp.maximum(margin, 0))
    passed = jax.random.randint(jax.random.fold_in(own, 4), (count // 2,), 0, 1 << 20) % (margin + 1)
    lengths = lengths.at[giver].add(-passed).at[receiver].add(passed)
    items = jnp.searchsorted(jnp.cumsum(lengths), jnp.arange(rows * top), side="right").astype(jnp.int32)
    listing = items.reshape(top, rows).T
    listing = listing[jax.random.permutation(jax.random.fold_in(own, 1), rows)]
    offset_by = jax.random.randint(jax.random.fold_in(own, 2), (rows, 1), 0, top)
    return jnp.take_along_axis(listing, (jnp.arange(top)[None, :] + offset_by) % top, axis=1)


def load_shares(count, total, bound, skew, full):
    loads = [(1 << 20) // math.isqrt(grade ** skew) + 1 for grade in range(1, count + 1)]
    largest = bound if full else min(bound, max(-(-total // count), total * loads[0] // sum(loads)))
    least = 1 if total - largest >= count - 1 else 0
    given, spare = [largest] + [least] * (count - 1), total - largest - least * (count - 1)
    while spare > 0:
        free = [i for i in range(1, count) if given[i] < largest] or [i for i in range(1, count) if given[i] < bound]
        mass, left = sum([loads[i] for i in free]), spare
        for i in free:
            addition = min(bound - given[i], max(1, left * loads[i] // mass), spare)
            given[i] = given[i] + addition
            spare = spare - addition
    return np.array(given)


def centred(own_key, shape, width, reach, pieces=(), held_as=jnp.bfloat16):
    loudness = shard_levels(own_key, shape, pieces, -0.22, 0.18) if pieces else 1.0
    values = jax.random.normal(own_key, shape, jnp.float32) * width * loudness
    return jnp.minimum(jnp.maximum(values, -reach), reach).astype(held_as)


def setup_inputs(seed: int = 0) -> dict:
    seeds = jax.random.split(jax.random.key(seed), 5)
    queries = draw_queries(jax.random.fold_in(seeds[4], 71), 0)
    keys = draw_keys(jax.random.fold_in(seeds[4], 71), 0)
    values = centred(seeds[2], (CONTEXT, KV_HEADS, HEAD_DIM), 1.0, 6.0, ((0, 32),))
    routes_keys = jax.random.split(jax.random.fold_in(seeds[3], 1), QUERIES // QRY_DEV)
    routes_turns = jax.random.permutation(jax.random.fold_in(seeds[3], 3), QUERIES // QRY_DEV)
    routes = jax.vmap(lambda own, number: shared_out(jax.random.fold_in(seeds[3], 2), own, number, QRY_DEV, HEADS, ROUTED, MOST, 2))(routes_keys, routes_turns).reshape((QUERIES, ROUTED))
    return {"queries": queries, "keys": keys, "values": values, "routes": routes}


def slot_index(routes_dev):
    flat_heads = routes_dev.reshape(-1)
    heads_all = jnp.arange(HEADS, dtype=jnp.int32)
    onehot = (flat_heads[:, None] == heads_all[None, :]).astype(jnp.int32)
    before = jnp.cumsum(onehot, axis=0) - onehot
    within = lax.optimization_barrier(jnp.sum(before * onehot, axis=1)).astype(jnp.int32)
    return (flat_heads * MOST + within).astype(jnp.int32)

def one_shard(arguments):
    device, query_dev, routes_dev, padded_keys, padded_values = arguments
    slots = slot_index(routes_dev)
    flat = query_dev.reshape(-1, HEAD_DIM)
    packed = jnp.zeros((HEADS * MOST, HEAD_DIM), jnp.float32).at[slots].set(flat.astype(jnp.float32))
    tokens_of = jnp.repeat(jnp.arange(QRY_DEV, dtype=jnp.int32), ROUTED)
    positions = jnp.zeros((HEADS * MOST,), jnp.int32).at[slots].set(tokens_of)
    packed = packed.reshape(KV_HEADS, -1, HEAD_DIM)
    positions = positions.reshape(KV_HEADS, -1)
    window = HOPS + 1
    start = (device * CTX_DEV).astype(jnp.int32)
    win_keys = lax.dynamic_slice_in_dim(padded_keys, start, window * CTX_DEV, 0).astype(jnp.float32)
    win_values = lax.dynamic_slice_in_dim(padded_values, start, window * CTX_DEV, 0).astype(jnp.float32)
    scores = jnp.einsum('gqd,kgd->gqk', packed, win_keys) / jnp.sqrt(jnp.float32(HEAD_DIM))
    column = jnp.arange(window * CTX_DEV, dtype=jnp.int32)
    shard_of = column // CTX_DEV
    inside = device - HOPS + shard_of >= 0
    offset = CTX_DEV - QRY_DEV
    causal = (shard_of < HOPS)[None, None, :] | ((column - HOPS * CTX_DEV)[None, None, :] <= (positions + offset)[:, :, None])
    allowed = inside[None, None, :] & causal
    scores = jnp.where(allowed, scores, jnp.float32(-1e+30))
    highest = lax.optimization_barrier(jnp.max(scores, axis=2))
    weights = jnp.where(allowed, jnp.exp(scores - highest[:, :, None]), jnp.float32(0.0))
    total = lax.optimization_barrier(jnp.sum(weights, axis=2))
    rounded = weights.astype(jnp.bfloat16).astype(jnp.float32)
    output = jnp.einsum('gqk,kgd->gqd', rounded, win_values) / total[:, :, None]
    output = output.astype(jnp.bfloat16).reshape(-1, HEAD_DIM)
    return output[slots].reshape(QRY_DEV, ROUTED, HEAD_DIM)

def reference(queries, keys, values, routes):
    shards = CONTEXT // CTX_DEV
    front = jnp.zeros((HOPS * CTX_DEV, KV_HEADS, HEAD_DIM), keys.dtype)
    padded_keys = jnp.concatenate([front, keys], axis=0)
    padded_values = jnp.concatenate([front, values], axis=0)
    query_all = queries.reshape(shards, QRY_DEV, ROUTED, HEAD_DIM)
    routes_all = routes.reshape(shards, QRY_DEV, ROUTED)
    devices = jnp.arange(shards, dtype=jnp.int32)
    result = lax.map(lambda item: one_shard((item[0], item[1], item[2], padded_keys, padded_values)), (devices, query_all, routes_all))
    return result.reshape(QUERIES, ROUTED, HEAD_DIM)
```

```python
import functools
import math

import jax
import jax.numpy as jnp
from jax import lax
from jax.experimental import pallas as pl
from jax.experimental.pallas import tpu as pltpu
from jax.sharding import PartitionSpec as P

HEADS = 64
HOPS = 4
MOST = 40
LANES = 128
LOW = -1e30
MESH = pl.DeviceIdType.MESH


def dot(a, b):
    return lax.dot_general(a, b, (((1,), (0,)), ((), ())), preferred_element_type=jnp.float32)


def dot_t(a, b):
    return lax.dot_general(a, b, (((1,), (1,)), ((), ())), preferred_element_type=jnp.float32)


def pack_kernel(groups, capacity, q_ref, routes_ref, packed_ref, pos_ref, slots_ref, wide):
    tokens, routed, width = q_ref.shape
    per_group = HEADS // groups
    wide[...] = q_ref[...].astype(jnp.float32)
    lane = lax.broadcasted_iota(jnp.int32, (tokens, LANES), 1)
    group_of = routes_ref[...] // per_group
    hots = [(group_of[:, r : r + 1] == lane).astype(jnp.float32) for r in range(routed)]
    count = functools.reduce(jnp.add, hots)
    row = lax.broadcasted_iota(jnp.int32, (tokens, tokens), 0)
    col = lax.broadcasted_iota(jnp.int32, (tokens, tokens), 1)
    lower = (col < row).astype(jnp.bfloat16)
    rank = dot(lower, count.astype(jnp.bfloat16)) + (lane * capacity).astype(jnp.float32)
    slots = jnp.zeros((tokens, LANES), jnp.float32)
    for r in range(routed):
        slot = jnp.sum(hots[r] * rank, axis=1, keepdims=True)
        slots = jnp.where(lane == r, slot, slots)
        rank = rank + hots[r]
    slots_ref[...] = slots.astype(jnp.int32)
    slots_t = slots.T.astype(jnp.int32)
    token = lax.broadcasted_iota(jnp.int32, (tokens, width), 0).astype(jnp.bfloat16)
    rights = [
        jnp.concatenate([wide[:, r, :].astype(jnp.bfloat16), token], axis=1) for r in range(routed)
    ]
    step = 256
    total = groups * capacity
    place = lax.broadcasted_iota(jnp.int32, (step, tokens), 0)
    for at in range(0, total, step):
        acc = jnp.zeros((step, 2 * width), jnp.float32)
        for r in range(routed):
            here = (place == slots_t[r : r + 1, :] - at).astype(jnp.float32).astype(jnp.bfloat16)
            acc = acc + dot(here, rights[r])
        packed_ref[pl.ds(at, step), :] = acc[:, :width].astype(jnp.bfloat16)
        pos_ref[pl.ds(at, step), :] = acc[:, width:]


def unpack_kernel(fin_ref, slots_ref, out_ref, wide):
    tokens, routed, width = out_ref.shape
    total = fin_ref.shape[0]
    lane = lax.broadcasted_iota(jnp.int32, (tokens, 256), 1)
    for r in range(routed):
        slot = slots_ref[:, r : r + 1]
        acc = jnp.zeros((tokens, width), jnp.float32)
        for at in range(0, total, 256):
            here = (lane == slot - at).astype(jnp.float32).astype(jnp.bfloat16)
            acc = acc + dot(here, fin_ref[pl.ds(at, 256), :])
        wide[:, r, :] = acc
    out_ref[...] = wide[...].astype(jnp.bfloat16)


def remote(src, dst, send, recv, device):
    return pltpu.make_async_remote_copy(
        src_ref=src, dst_ref=dst, send_sem=send, recv_sem=recv,
        device_id=(device,), device_id_type=MESH,
    )


def attend(q, k, v, scale, mask=None):
    s = dot_t(q, k) * scale
    if mask is not None:
        s = mask(s)
    top = jnp.max(s, axis=1, keepdims=True)
    p = jnp.exp2(s - top).astype(jnp.bfloat16)
    ones = jnp.ones(v.shape, jnp.bfloat16)
    both = dot(p, jnp.concatenate([v, ones], axis=1))
    width = v.shape[1]
    total = both[:, width:]
    return both[:, :width] / total, top + jnp.log2(total)


def main_kernel(
    n, q, pos, k8, v8, fin, kh, vh, qb, qc, qd, oa, ob, oc, od, rb, rc, rd,
    st, ts, rs_b, rs_c, rs_d, kv_send, kv_recv, kv_local, qb_sem, qc_send, qc_recv,
    qd_send, qd_recv, ob_sem, oc_send, oc_recv, od_send, od_recv, sb_sem, sc_send, sc_recv,
    sd_send, sd_recv,
):
    groups, capacity, width = q.shape
    context = k8.shape[1]
    tokens = context // 2
    half = groups // 2
    chips = n // 2
    me = lax.axis_index("seq")
    c = me // 2
    k = me % 2
    other = 1 - k
    partner = c * 2 + other
    scale = jnp.float32(math.log2(math.e) / math.sqrt(width))
    exists = {-2: c >= 2, -1: c >= 1, 1: c + 1 < chips, 2: c + 2 < chips}

    barrier = pltpu.get_barrier_semaphore()

    def signal(device):
        pl.semaphore_signal(barrier, inc=1, device_id=(device,), device_id_type=MESH)

    signal(partner)
    for far, there in exists.items():
        @pl.when(there)
        def _(far=far):
            signal((c + far) * 2)
            signal((c + far) * 2 + 1)
    peers = 1
    for there in exists.values():
        peers = peers + 2 * there.astype(jnp.int32)
    pl.semaphore_wait(barrier, peers)

    def query_copy(x, s, r, far, g8):
        j, g = g8 // half, g8 % half
        return remote(q.at[g8], x.at[k, g], s.at[g8], r.at[k, g], (c - far) * 2 + j)

    order = [j * half + g for g in range(half) for j in range(2)]
    for g8 in order:
        @pl.when(exists[-1])
        def _(g8=g8):
            query_copy(qc, qc_send, qc_recv, 1, g8).start()
        @pl.when(exists[-2])
        def _(g8=g8):
            query_copy(qd, qd_send, qd_recv, 2, g8).start()

    def kv_copies():
        return [
            remote(a.at[pl.ds(other * half, half)], b.at[k], kv_send.at[i], kv_recv.at[i], partner)
            for i, (a, b) in enumerate(((k8, kh), (v8, vh)))
        ]

    def kv_locals():
        return [
            pltpu.make_async_copy(a.at[pl.ds(k * half, half)], b.at[k], kv_local.at[i])
            for i, (a, b) in enumerate(((k8, kh), (v8, vh)))
        ]

    for one in kv_copies() + kv_locals():
        one.start()

    def qb_copy():
        return remote(q.at[pl.ds(0, half)], qb, qb_sem.at[0], qb_sem.at[1], partner)

    @pl.when(k == 1)
    def _():
        qb_copy().start()

    lane = lax.broadcasted_iota(jnp.int32, (capacity, LANES), 1)

    def keep(at, i, lse):
        st[at, pl.ds(0, capacity), :] = jnp.where(lane == i, lse, st[at, pl.ds(0, capacity), :])

    st[...] = jnp.full(st.shape, LOW, jnp.float32)

    column = lax.broadcasted_iota(jnp.int32, (capacity, tokens), 1).astype(jnp.float32)

    def own(g, carry):
        at = pos[g]
        limit = jnp.concatenate([at] * (tokens // LANES), axis=1)

        def mask(s):
            tail = jnp.where(column <= limit, s[:, context - tokens :], jnp.float32(LOW))
            return jnp.concatenate([s[:, : context - tokens], tail], axis=1)

        o, lse = attend(q[g], k8[g], v8[g], scale, mask)
        oa[g] = o
        keep(0, g, lse)
        return carry

    lax.fori_loop(0, groups, own, 0)

    for one in kv_copies():
        one.wait_recv()
    for one in kv_locals():
        one.wait()

    def stat_copies(slot, i, r, s_sem, r_sem, device):
        return remote(ts.at[slot], r.at[i], s_sem, r_sem, device)

    def second(queries, at):
        def body(g, carry):
            o, lse = attend(queries(g), kh[0, g], vh[0, g], scale)
            ob[g] = o.astype(jnp.bfloat16)
            keep(1, at + g, lse)
            return carry
        lax.fori_loop(0, half, body, 0)

    def ob_copies():
        return [
            remote(ob, rb, ob_sem.at[0], ob_sem.at[1], partner),
            remote(ts.at[0], rs_b, sb_sem.at[0], sb_sem.at[1], partner),
        ]

    @pl.when(k == 0)
    def _():
        qb_copy().wait_recv()
        second(lambda g: qb[g], 0)
        ts[0] = st[1].T[:8]
        for one in ob_copies():
            one.start()

    @pl.when(k == 1)
    def _():
        second(lambda g: q[half + g], half)

    def out_copy(o, r, s_sem, r_sem, far, j, g):
        return remote(o.at[j, g], r.at[k * half + g], s_sem.at[j, g], r_sem.at[k * half + g], (c + far) * 2 + j)

    def stat_copy(slot, r, s_sem, r_sem, far, j):
        return remote(ts.at[slot + j], r.at[k], s_sem.at[j], r_sem.at[k], (c + far) * 2 + j)

    def serve(far, j, g, x, x_send, x_recv, o, o_send, r, r_recv, at, part):
        remote(x.at[j, g], x.at[j, g], x_send.at[0], x_recv.at[j, g], partner).wait_recv()
        if part:
            keys, values = kh[1, g], vh[1, g]
        else:
            keys = jnp.concatenate([kh[0, g], kh[1, g]], axis=0)
            values = jnp.concatenate([vh[0, g], vh[1, g]], axis=0)
        out, lse = attend(x[j, g], keys, values, scale)
        o[j, g] = out.astype(jnp.bfloat16)
        keep(at, g, lse)
        out_copy(o, r, o_send, r_recv, far, j, g).start()

    @pl.when(exists[1])
    def _():
        def body(i, carry):
            g, j = i // 2, i % 2
            serve(1, j, g, qc, qc_send, qc_recv, oc, oc_send, rc, oc_recv, 2 + j, False)
            return carry
        lax.fori_loop(0, groups, body, 0)
        for j in range(2):
            ts[1 + j] = st[2 + j].T[:8]
            stat_copy(1, rs_c, sc_send, sc_recv, 1, j).start()

    @pl.when(exists[2])
    def _():
        def body(g, carry):
            for j in range(2):
                serve(2, j, g, qd, qd_send, qd_recv, od, od_send, rd, od_recv, 4 + j, j == 1)
            return carry
        lax.fori_loop(0, half, body, 0)
        for j in range(2):
            ts[3 + j] = st[4 + j].T[:8]
            stat_copy(3, rs_d, sd_send, sd_recv, 2, j).start()

    for far, r, rs, r_recv, s_recv, o, o_send, s_send in (
        (1, rc, rs_c, oc_recv, sc_recv, oc, oc_send, sc_send),
        (2, rd, rs_d, od_recv, sd_recv, od, od_send, sd_send),
    ):
        @pl.when(exists[-far])
        def _(r=r, rs=rs, r_recv=r_recv, s_recv=s_recv, o=o, o_send=o_send, s_send=s_send):
            for g8 in range(groups):
                remote(o.at[0, 0], r.at[g8], o_send.at[0, 0], r_recv.at[g8], partner).wait_recv()
            for j in range(2):
                remote(ts.at[0], rs.at[j], s_send.at[0], s_recv.at[j], partner).wait_recv()

        @pl.when(jnp.logical_not(exists[-far]))
        def _(r=r, rs=rs):
            r[...] = jnp.zeros(r.shape, r.dtype)
            rs[...] = jnp.full(rs.shape, LOW, rs.dtype)

    @pl.when(k == 1)
    def _():
        for one in ob_copies():
            one.wait_recv()

    @pl.when(k == 0)
    def _():
        rb[...] = jnp.zeros(rb.shape, rb.dtype)
        rs_b[...] = jnp.full(rs_b.shape, LOW, rs_b.dtype)

    padded = st.shape[1]
    for h in range(2):
        tiles = [rs_c[h], rs_d[h]] + ([rs_b[...]] if h == 0 else [])
        pad = jnp.full((LANES - 8 * len(tiles), padded), LOW, jnp.float32)
        turned = jnp.concatenate(tiles + [pad], axis=0).T
        for g in range(half):
            g8 = h * half + g
            lse_a = st[0, pl.ds(0, capacity), g8 : g8 + 1]
            lse_c = turned[:capacity, g : g + 1]
            lse_d = turned[:capacity, 8 + g : 9 + g]
            if h == 0:
                lse_b = turned[:capacity, 16 + g : 17 + g]
                o_b = rb[g].astype(jnp.float32)
            else:
                kept = st[1, pl.ds(0, capacity), g8 : g8 + 1]
                lse_b = jnp.where(k == 1, kept, jnp.float32(LOW))
                o_b = ob[g].astype(jnp.float32)
            top = jnp.maximum(jnp.maximum(lse_a, lse_b), jnp.maximum(lse_c, lse_d))
            w_a, w_b, w_c, w_d = (jnp.exp2(x - top) for x in (lse_a, lse_b, lse_c, lse_d))
            inverse = 1.0 / (w_a + w_b + w_c + w_d)
            merged = (
                oa[g8] * (w_a * inverse)
                + o_b * (w_b * inverse)
                + rc[g8].astype(jnp.float32) * (w_c * inverse)
                + rd[g8].astype(jnp.float32) * (w_d * inverse)
            )
            fin[g8] = merged.astype(jnp.bfloat16)

    for one in kv_copies():
        one.wait_send()

    @pl.when(k == 1)
    def _():
        qb_copy().wait_send()

    @pl.when(k == 0)
    def _():
        for one in ob_copies():
            one.wait_send()

    for far, x, s, r in ((1, qc, qc_send, qc_recv), (2, qd, qd_send, qd_recv)):
        @pl.when(exists[-far])
        def _(far=far, x=x, s=s, r=r):
            for g8 in range(groups):
                query_copy(x, s, r, far, g8).wait_send()

    for far, o, r, o_send, r_recv, slot, rs, s_send, s_recv in (
        (1, oc, rc, oc_send, oc_recv, 1, rs_c, sc_send, sc_recv),
        (2, od, rd, od_send, od_recv, 3, rs_d, sd_send, sd_recv),
    ):
        @pl.when(exists[far])
        def _(far=far, o=o, r=r, o_send=o_send, r_recv=r_recv, slot=slot, rs=rs, s_send=s_send, s_recv=s_recv):
            for j in range(2):
                for g in range(half):
                    out_copy(o, r, o_send, r_recv, far, j, g).wait_send()
                stat_copy(slot, rs, s_send, s_recv, far, j).wait_send()


def shards(n, queries, keys, values, routes):
    tokens, routed, width = queries.shape
    context, groups, _ = keys.shape
    capacity = HEADS // groups * MOST
    half = groups // 2
    padded = -(-capacity // LANES) * LANES
    total = groups * capacity
    vmem = pl.BlockSpec(memory_space=pltpu.VMEM)
    packed, pos, slots = pl.pallas_call(
        functools.partial(pack_kernel, groups, capacity),
        out_shape=(
            jax.ShapeDtypeStruct((total, width), jnp.bfloat16),
            jax.ShapeDtypeStruct((total, width), jnp.float32),
            jax.ShapeDtypeStruct((tokens, LANES), jnp.int32),
        ),
        in_specs=[vmem] * 2,
        out_specs=(vmem,) * 3,
        scratch_shapes=[pltpu.VMEM((tokens, routed, width), jnp.float32)],
        name="pack",
    )(queries, routes)
    k8 = keys.transpose(1, 0, 2)
    v8 = values.transpose(1, 0, 2)
    bf = lambda *shape: pltpu.VMEM(shape, jnp.bfloat16)
    f32 = lambda *shape: pltpu.VMEM(shape, jnp.float32)
    sem = lambda *shape: pltpu.SemaphoreType.DMA(shape)
    fin = pl.pallas_call(
        functools.partial(main_kernel, n),
        out_shape=jax.ShapeDtypeStruct((groups, capacity, width), jnp.bfloat16),
        in_specs=[vmem] * 4,
        out_specs=vmem,
        scratch_shapes=[
            bf(2, half, context, width),
            bf(2, half, context, width),
            bf(half, capacity, width),
            bf(2, half, capacity, width),
            bf(2, half, capacity, width),
            f32(groups, capacity, width),
            bf(half, capacity, width),
            bf(2, half, capacity, width),
            bf(2, half, capacity, width),
            bf(half, capacity, width),
            bf(groups, capacity, width),
            bf(groups, capacity, width),
            f32(6, padded, LANES),
            f32(5, 8, padded),
            f32(8, padded),
            f32(2, 8, padded),
            f32(2, 8, padded),
            sem(2), sem(2), sem(2), sem(2),
            sem(groups), sem(2, half), sem(groups), sem(2, half),
            sem(2), sem(2, half), sem(groups), sem(2, half), sem(groups),
            sem(2), sem(2), sem(2), sem(2), sem(2),
        ],
        compiler_params=pltpu.CompilerParams(
            collective_id=0, has_side_effects=True, vmem_limit_bytes=60 * 1024 * 1024
        ),
        name="main",
    )(packed.reshape(groups, capacity, width), pos.reshape(groups, capacity, width), k8, v8)
    return pl.pallas_call(
        unpack_kernel,
        out_shape=jax.ShapeDtypeStruct((tokens, routed, width), jnp.bfloat16),
        in_specs=[vmem] * 2,
        out_specs=vmem,
        scratch_shapes=[pltpu.VMEM((tokens, routed, width), jnp.float32)],
        name="unpack",
    )(fin.reshape(total, width), slots)


def solution(mesh):
    n = mesh.shape["seq"]
    placed = (P("seq", None, None), P("seq", None, None), P("seq", None, None), P("seq", None))
    return jax.shard_map(
        functools.partial(shards, n),
        mesh=mesh,
        in_specs=placed,
        out_specs=P("seq", None, None),
        check_vma=False,
    )
```

```python
import functools
import math

import jax
import jax.numpy as jnp
from jax import lax
from jax.experimental import pallas as pl
from jax.experimental.pallas import tpu as pltpu
from jax.sharding import PartitionSpec as P

HEADS = 64
HOPS = 4
MOST = 40
LANES = 128
LOW = -1e30
MESH = pl.DeviceIdType.MESH


def dot(a, b):
    return lax.dot_general(a, b, (((1,), (0,)), ((), ())), preferred_element_type=jnp.float32)


def dot_t(a, b):
    return lax.dot_general(a, b, (((1,), (1,)), ((), ())), preferred_element_type=jnp.float32)


def pack_kernel(groups, capacity, q_ref, routes_ref, packed_ref, pos_ref, slots_ref, wide):
    tokens, routed, width = q_ref.shape
    per_group = HEADS // groups
    wide[...] = q_ref[...].astype(jnp.float32)
    lane = lax.broadcasted_iota(jnp.int32, (tokens, LANES), 1)
    turned = routes_ref[...].astype(jnp.float32)
    group_of = jnp.concatenate([turned] * (LANES // routed), axis=0).T.astype(jnp.int32) // per_group
    hots = [(group_of[:, r : r + 1] == lane).astype(jnp.float32) for r in range(routed)]
    count = functools.reduce(jnp.add, hots)
    row = lax.broadcasted_iota(jnp.int32, (tokens, tokens), 0)
    col = lax.broadcasted_iota(jnp.int32, (tokens, tokens), 1)
    lower = (col < row).astype(jnp.bfloat16)
    rank = dot(lower, count.astype(jnp.bfloat16)) + (lane * capacity).astype(jnp.float32)
    slots = jnp.zeros((tokens, LANES), jnp.float32)
    for r in range(routed):
        slot = jnp.sum(hots[r] * rank, axis=1, keepdims=True)
        slots = jnp.where(lane == r, slot, slots)
        rank = rank + hots[r]
    slots_ref[...] = slots.astype(jnp.int32)
    slots_t = slots.T.astype(jnp.int32)
    token = lax.broadcasted_iota(jnp.int32, (tokens, width), 0).astype(jnp.bfloat16)
    rights = [
        jnp.concatenate([wide[:, r, :].astype(jnp.bfloat16), token], axis=1) for r in range(routed)
    ]
    step = 256
    total = groups * capacity
    place = lax.broadcasted_iota(jnp.int32, (step, tokens), 0)
    for at in range(0, total, step):
        acc = jnp.zeros((step, 2 * width), jnp.float32)
        for r in range(routed):
            here = (place == slots_t[r : r + 1, :] - at).astype(jnp.float32).astype(jnp.bfloat16)
            acc = acc + dot(here, rights[r])
        packed_ref[pl.ds(at, step), :] = acc[:, :width].astype(jnp.bfloat16)
        pos_ref[pl.ds(at, step), :] = acc[:, width:]


def unpack_kernel(fin_ref, slots_ref, out_ref, wide):
    tokens, routed, width = out_ref.shape
    total = fin_ref.shape[0]
    lane = lax.broadcasted_iota(jnp.int32, (tokens, 256), 1)
    for r in range(routed):
        slot = slots_ref[:, r : r + 1]
        acc = jnp.zeros((tokens, width), jnp.float32)
        for at in range(0, total, 256):
            here = (lane == slot - at).astype(jnp.float32).astype(jnp.bfloat16)
            acc = acc + dot(here, fin_ref[pl.ds(at, 256), :])
        wide[:, r, :] = acc
    out_ref[...] = wide[...].astype(jnp.bfloat16)


def remote(src, dst, send, recv, device):
    return pltpu.make_async_remote_copy(
        src_ref=src, dst_ref=dst, send_sem=send, recv_sem=recv,
        device_id=(device,), device_id_type=MESH,
    )


def attend(q, k, v, scale, mask=None):
    s = dot_t(q, k) * scale
    if mask is not None:
        s = mask(s)
    top = jnp.max(s, axis=1, keepdims=True)
    p = jnp.exp2(s - top).astype(jnp.bfloat16)
    ones = jnp.ones(v.shape, jnp.bfloat16)
    both = dot(p, jnp.concatenate([v, ones], axis=1))
    width = v.shape[1]
    total = both[:, width:]
    return both[:, :width] / total, top + jnp.log2(total)


def squeeze(lse, padded):
    rows = lse.shape[0]
    return jnp.concatenate([lse, jnp.zeros((padded - rows, LANES), jnp.float32)], axis=0).T[:8]


def widen(tile, rows):
    return jnp.concatenate([tile] * (LANES // 8), axis=0).T[:rows]


def merge(parts):
    top = functools.reduce(jnp.maximum, [lse for _, lse in parts])
    weights = [jnp.exp2(lse - top) for _, lse in parts]
    total = functools.reduce(jnp.add, weights)
    mixed = functools.reduce(jnp.add, [o.astype(jnp.float32) * w for (o, _), w in zip(parts, weights)])
    return mixed / total, top + jnp.log2(total)


def main_kernel(
    n, q, pos, k8, v8, fin, kh, vh, qb, qc, qd, oa, la, ob, lb, tb, rb, sb,
    oc, tc, od, ld, td, rx, sx, rc, sc, rd, sd,
    kv_send, kv_recv, kv_local, qb_sem, qc_send, qc_recv, qd_send, qd_recv, relay_send,
    ob_send, ob_recv, tb_send, tb_recv, oc_send, tc_send, od_send, td_send,
    rx_recv, sx_recv, rc_recv, sc_recv, rd_recv, sd_recv,
):
    groups, capacity, width = q.shape
    context = k8.shape[1]
    tokens = context // 2
    padded = tb.shape[2]
    half = groups // 2
    chips = n // 2
    me = lax.axis_index("seq")
    c = me // 2
    k = me % 2
    other = 1 - k
    partner = c * 2 + other
    even = c % 2 == 0
    odd = c % 2 == 1
    scale = jnp.float32(math.log2(math.e) / math.sqrt(width))
    exists = {-2: c >= 2, -1: c >= 1, 1: c + 1 < chips, 2: c + 2 < chips}
    near = jnp.logical_and(odd, exists[-1])

    barrier = pltpu.get_barrier_semaphore()

    def signal(device):
        pl.semaphore_signal(barrier, inc=1, device_id=(device,), device_id_type=MESH)

    signal(partner)
    peers = 1
    for far, there in exists.items():
        @pl.when(there)
        def _(far=far):
            signal((c + far) * 2)
            signal((c + far) * 2 + 1)
        peers = peers + 2 * there.astype(jnp.int32)
    pl.semaphore_wait(barrier, peers)

    def query_copy(x, s, r, far, g8):
        j, g = g8 // half, g8 % half
        return remote(q.at[g8], x.at[k, g], s.at[g8], r.at[k, g], (c - far) * 2 + j)

    for g8 in [j * half + g for g in range(half) for j in range(2)]:
        @pl.when(exists[-2])
        def _(g8=g8):
            query_copy(qd, qd_send, qd_recv, 2, g8).start()
        @pl.when(near)
        def _(g8=g8):
            query_copy(qc, qc_send, qc_recv, 1, g8).start()

    def kv_copies():
        return [
            remote(a.at[pl.ds(other * half, half)], b.at[k], kv_send.at[i], kv_recv.at[i], partner)
            for i, (a, b) in enumerate(((k8, kh), (v8, vh)))
        ]

    def kv_locals():
        return [
            pltpu.make_async_copy(a.at[pl.ds(k * half, half)], b.at[k], kv_local.at[i])
            for i, (a, b) in enumerate(((k8, kh), (v8, vh)))
        ]

    for one in kv_copies() + kv_locals():
        one.start()

    def qb_copy():
        return remote(q.at[pl.ds(0, half)], qb, qb_sem.at[0], qb_sem.at[1], partner)

    @pl.when(k == 1)
    def _():
        qb_copy().start()

    column = lax.broadcasted_iota(jnp.int32, (capacity, tokens), 1).astype(jnp.float32)

    def own(g, carry):
        limit = jnp.concatenate([pos[g]] * (tokens // LANES), axis=1)

        def mask(s):
            tail = jnp.where(column <= limit, s[:, context - tokens :], jnp.float32(LOW))
            return jnp.concatenate([s[:, : context - tokens], tail], axis=1)

        oa[g], la[g] = attend(q[g], k8[g], v8[g], scale, mask)
        return carry

    lax.fori_loop(0, groups, own, 0)

    for one in kv_copies():
        one.wait_recv()
    for one in kv_locals():
        one.wait()

    @pl.when(k == 0)
    def _():
        qb_copy().wait_recv()

    def b_copies(g):
        return (
            remote(ob.at[g], rb.at[g], ob_send.at[g], ob_recv.at[g], partner),
            remote(tb.at[g], sb.at[g], tb_send.at[g], tb_recv.at[g], partner),
        )

    def c_near(j, g):
        at = k * half + g
        to = (c + 1) * 2 + j
        return (
            remote(oc.at[j, g], rc.at[at], oc_send.at[j, g], rc_recv.at[at], to),
            remote(tc.at[j, g], sc.at[at], tc_send.at[j, g], sc_recv.at[at], to),
        )

    def c_relay(j, g):
        to = (c - 1) * 2 + k
        return (
            remote(oc.at[j, g], rx.at[j, g], oc_send.at[j, g], rx_recv.at[j, g], to),
            remote(tc.at[j, g], sx.at[j, g], tc_send.at[j, g], sx_recv.at[j, g], to),
        )

    def d_copies(j, g):
        at = k * half + g
        to = (c + 2) * 2 + j
        return (
            remote(od.at[j, g], rd.at[at], od_send.at[j, g], rd_recv.at[at], to),
            remote(td.at[j, g], sd.at[at], td_send.at[j, g], sd_recv.at[at], to),
        )

    def query_relay(j, g):
        return remote(
            qd.at[j, g], qc.at[j, g], relay_send.at[j, g], qc_recv.at[j, g], (c + 1) * 2 + k
        )

    def start(copies):
        for one in copies:
            one.start()

    def both(x, g):
        return jnp.concatenate([x[0, g], x[1, g]], axis=0)

    lag, delay = 1, 3

    def step(i, carry):
        @pl.when(jnp.logical_and(i < groups, exists[2]))
        def _():
            g, j = i // 2, i % 2
            remote(qd.at[j, g], qd.at[j, g], qd_send.at[0], qd_recv.at[j, g], partner).wait_recv()

            @pl.when(even)
            def _():
                query_relay(j, g).start()

            def put(out, lse):
                od[j, g] = out.astype(jnp.bfloat16)
                ld[j, g] = lse

            @pl.when(j == 0)
            def _():
                put(*attend(qd[j, g], both(kh, g), both(vh, g), scale))

            @pl.when(j == 1)
            def _():
                put(*attend(qd[j, g], kh[1, g], vh[1, g], scale))

            @pl.when(odd)
            def _():
                td[j, g] = squeeze(ld[j, g], padded)
                start(d_copies(j, g))

        @pl.when(i < half)
        def _():
            @pl.when(k == 1)
            def _():
                qb[i] = q[half + i]

            out, lse = attend(qb[i], kh[0, i], vh[0, i], scale)
            ob[i] = out.astype(jnp.bfloat16)
            lb[i] = lse

            @pl.when(k == 0)
            def _():
                tb[i] = squeeze(lse, padded)
                start(b_copies(i))

        @pl.when(jnp.logical_and(jnp.logical_and(i >= lag, i < groups + lag), exists[1]))
        def _():
            at = i - lag
            g, j = at // 2, at % 2
            remote(qc.at[j, g], qc.at[j, g], qc_send.at[0], qc_recv.at[j, g], partner).wait_recv()
            out, lse = attend(qc[j, g], both(kh, g), both(vh, g), scale)
            oc[j, g] = out.astype(jnp.bfloat16)
            tc[j, g] = squeeze(lse, padded)

            @pl.when(even)
            def _():
                start(c_near(j, g))

            @pl.when(odd)
            def _():
                start(c_relay(j, g))

        @pl.when(jnp.logical_and(jnp.logical_and(i >= delay, even), exists[2]))
        def _():
            at = i - delay
            g, j = at // 2, at % 2
            remote(oc.at[j, g], rx.at[j, g], oc_send.at[j, g], rx_recv.at[j, g], partner).wait_recv()
            remote(tc.at[j, g], sx.at[j, g], tc_send.at[j, g], sx_recv.at[j, g], partner).wait_recv()
            out, lse = merge([(od[j, g], ld[j, g]), (rx[j, g], widen(sx[j, g], capacity))])
            od[j, g] = out.astype(jnp.bfloat16)
            td[j, g] = squeeze(lse, padded)
            start(d_copies(j, g))

        return carry

    lax.fori_loop(0, groups + delay, step, 0)

    def absent(o, t):
        o[...] = jnp.zeros(o.shape, o.dtype)
        t[...] = jnp.full(t.shape, LOW, t.dtype)

    @pl.when(jnp.logical_not(near))
    def _():
        absent(rc, sc)

    @pl.when(jnp.logical_not(exists[-2]))
    def _():
        absent(rd, sd)

    @pl.when(k == 0)
    def _():
        absent(rb, sb)

    def finish(g8, carry):
        @pl.when(near)
        def _():
            remote(oc.at[0, 0], rc.at[g8], oc_send.at[0, 0], rc_recv.at[g8], partner).wait_recv()
            remote(tc.at[0, 0], sc.at[g8], tc_send.at[0, 0], sc_recv.at[g8], partner).wait_recv()

        @pl.when(exists[-2])
        def _():
            remote(od.at[0, 0], rd.at[g8], od_send.at[0, 0], rd_recv.at[g8], partner).wait_recv()
            remote(td.at[0, 0], sd.at[g8], td_send.at[0, 0], sd_recv.at[g8], partner).wait_recv()

        parts = [
            (oa[g8], la[g8]), (rc[g8], widen(sc[g8], capacity)), (rd[g8], widen(sd[g8], capacity))
        ]
        second = jnp.logical_and(k == 1, g8 < half)

        @pl.when(second)
        def _():
            for one in b_copies(g8 % half):
                one.wait_recv()
            g = g8 % half
            fin[g8] = merge(parts + [(rb[g], widen(sb[g], capacity))])[0].astype(jnp.bfloat16)

        @pl.when(jnp.logical_not(second))
        def _():
            g = g8 % half
            lse = jnp.where(k == 1, lb[g], jnp.float32(LOW))
            fin[g8] = merge(parts + [(ob[g], lse)])[0].astype(jnp.bfloat16)

        return carry

    lax.fori_loop(0, groups, finish, 0)

    for one in kv_copies():
        one.wait_send()

    @pl.when(k == 1)
    def _():
        qb_copy().wait_send()

    def sent(there, make):
        @pl.when(there)
        def _():
            for j in range(2):
                for g in range(half):
                    for one in make(j, g):
                        one.wait_send()

    @pl.when(k == 0)
    def _():
        for g in range(half):
            for one in b_copies(g):
                one.wait_send()

    sent(exists[-2], lambda j, g: (query_copy(qd, qd_send, qd_recv, 2, j * half + g),))
    sent(near, lambda j, g: (query_copy(qc, qc_send, qc_recv, 1, j * half + g),))
    sent(jnp.logical_and(even, exists[2]), lambda j, g: (query_relay(j, g),))
    sent(exists[2], d_copies)
    sent(jnp.logical_and(even, exists[1]), c_near)
    sent(jnp.logical_and(odd, exists[1]), c_relay)


def shards(n, queries, keys, values, routes):
    tokens, routed, width = queries.shape
    context, groups, _ = keys.shape
    capacity = HEADS // groups * MOST
    half = groups // 2
    padded = -(-capacity // LANES) * LANES
    total = groups * capacity
    vmem = pl.BlockSpec(memory_space=pltpu.VMEM)
    packed, pos, slots = pl.pallas_call(
        functools.partial(pack_kernel, groups, capacity),
        out_shape=(
            jax.ShapeDtypeStruct((total, width), jnp.bfloat16),
            jax.ShapeDtypeStruct((total, width), jnp.float32),
            jax.ShapeDtypeStruct((tokens, LANES), jnp.int32),
        ),
        in_specs=[vmem] * 2,
        out_specs=(vmem,) * 3,
        scratch_shapes=[pltpu.VMEM((tokens, routed, width), jnp.float32)],
        name="pack",
    )(queries, routes.T)
    k8 = keys.transpose(1, 0, 2)
    v8 = values.transpose(1, 0, 2)
    bf = lambda *shape: pltpu.VMEM(shape, jnp.bfloat16)
    f32 = lambda *shape: pltpu.VMEM(shape, jnp.float32)
    sem = lambda *shape: pltpu.SemaphoreType.DMA(shape)
    chunks = lambda: bf(2, half, capacity, width)
    fin = pl.pallas_call(
        functools.partial(main_kernel, n),
        out_shape=jax.ShapeDtypeStruct((groups, capacity, width), jnp.bfloat16),
        in_specs=[vmem] * 4,
        out_specs=vmem,
        scratch_shapes=[
            bf(2, half, context, width), bf(2, half, context, width),
            bf(half, capacity, width), chunks(), chunks(),
            f32(groups, capacity, width), f32(groups, capacity, width),
            bf(half, capacity, width), f32(half, capacity, width), f32(half, 8, padded),
            bf(half, capacity, width), f32(half, 8, padded),
            chunks(), f32(2, half, 8, padded),
            chunks(), f32(2, half, capacity, width), f32(2, half, 8, padded),
            chunks(), f32(2, half, 8, padded),
            bf(groups, capacity, width), f32(groups, 8, padded),
            bf(groups, capacity, width), f32(groups, 8, padded),
            sem(2), sem(2), sem(2), sem(2),
            sem(groups), sem(2, half), sem(groups), sem(2, half), sem(2, half),
            sem(half), sem(half), sem(half), sem(half),
            sem(2, half), sem(2, half), sem(2, half), sem(2, half),
            sem(2, half), sem(2, half), sem(groups), sem(groups), sem(groups), sem(groups),
        ],
        compiler_params=pltpu.CompilerParams(
            collective_id=0, has_side_effects=True, vmem_limit_bytes=60 * 1024 * 1024
        ),
        name="main",
    )(packed.reshape(groups, capacity, width), pos.reshape(groups, capacity, width), k8, v8)
    return pl.pallas_call(
        unpack_kernel,
        out_shape=jax.ShapeDtypeStruct((tokens, routed, width), jnp.bfloat16),
        in_specs=[vmem] * 2,
        out_specs=vmem,
        scratch_shapes=[pltpu.VMEM((tokens, routed, width), jnp.float32)],
        name="unpack",
    )(fin.reshape(total, width), slots)


def solution(mesh):
    n = mesh.shape["seq"]
    placed = (P("seq", None, None), P("seq", None, None), P("seq", None, None), P("seq", None))
    return jax.shard_map(
        functools.partial(shards, n),
        mesh=mesh,
        in_specs=placed,
        out_specs=P("seq", None, None),
        check_vma=False,
    )
```
